32 devices in a mesh: ctx: 8 (over z, y), tp: 4 (over x, core).
Axes of the slice: x: 2, y: 2, z: 4, core: 2. Of those that a mesh axis runs over, the one named last changes fastest.
Arguments:
- tokens_in: bfloat16 [4, 2048, 2048], P(None, 'ctx'), may hold values from -6 to 6
- query_weight: bfloat16 [2048, 2048], P('ctx', 'tp'), may hold values from -0.125 to 0.125
- key_weight: bfloat16 [2048, 256], P('ctx', 'tp'), may hold values from -0.125 to 0.125
- value_weight: bfloat16 [2048, 256], P('ctx', 'tp'), may hold values from -0.125 to 0.125
- output_projection_matrix: bfloat16 [2048, 2048], P('tp', 'ctx'), may hold values from -1 to 1
- gate_weight: bfloat16 [2048, 5632], P('ctx', 'tp'), may hold values from -0.125 to 0.125
- up_weight: bfloat16 [2048, 5632], P('ctx', 'tp'), may hold values from -0.125 to 0.125
- down_projection_matrix: bfloat16 [5632, 2048], P('tp', 'ctx'), may hold values from -0.078125 to 0.078125
- gain_attn: bfloat16 [2048], replicated, may hold values from 0.099609375 to 1.8984375
- gain_ffn: bfloat16 [2048], replicated, may hold values from 0.099609375 to 1.8984375
- query_in: bfloat16 [8, 2048, 16], replicated, may hold values from -0.125 to 0.125
- query_out: bfloat16 [8, 16, 2048], P(None, None, 'tp'), may hold values from -0.375 to 0.375
- key_in: bfloat16 [8, 2048, 16], replicated, may hold values from -0.125 to 0.125
- key_out: bfloat16 [8, 16, 256], P(None, None, 'tp'), may hold values from -0.375 to 0.375
- value_in: bfloat16 [8, 2048, 16], replicated, may hold values from -0.125 to 0.125
- value_out: bfloat16 [8, 16, 256], P(None, None, 'tp'), may hold values from -0.375 to 0.375
- output_in: bfloat16 [8, 2048, 16], P(None, 'tp'), may hold values from -1 to 1
- output_adapter_second: bfloat16 [8, 16, 2048], replicated, may hold values from -0.375 to 0.375
- gate_in: bfloat16 [8, 2048, 16], replicated, may hold values from -0.125 to 0.125
- gate_out: bfloat16 [8, 16, 5632], P(None, None, 'tp'), may hold values from -0.375 to 0.375
- up_in: bfloat16 [8, 2048, 16], replicated, may hold values from -0.125 to 0.125
- up_out: bfloat16 [8, 16, 5632], P(None, None, 'tp'), may hold values from -0.375 to 0.375
- down_in: bfloat16 [8, 5632, 16], P(None, 'tp'), may hold values from -0.078125 to 0.078125
- down_adapter_second: bfloat16 [8, 16, 2048], replicated, may hold values from -0.375 to 0.375
- adapter_index: int32 [4], replicated, may hold values from 0 to 7
- cotangent: bfloat16 [4, 2048, 2048], P(None, 'ctx'), may hold values from -6 to 6
Outputs:
- output: bfloat16 [4, 2048, 2048], P(None, 'ctx')
- grad_tokens: bfloat16 [4, 2048, 2048], P(None, 'ctx')
- grad_query_in: float32 [8, 2048, 16], P(None, ('ctx', 'tp'))
- grad_query_out: float32 [8, 16, 2048], P(None, None, 'tp')
- grad_key_in: float32 [8, 2048, 16], P(None, ('ctx', 'tp'))
- grad_key_out: float32 [8, 16, 256], P(None, None, 'tp')
- grad_value_in: float32 [8, 2048, 16], P(None, ('ctx', 'tp'))
- grad_value_out: float32 [8, 16, 256], P(None, None, 'tp')
- grad_output_in: float32 [8, 2048, 16], P(None, 'tp')
- grad_output_out: float32 [8, 16, 2048], replicated
- grad_gate_in: float32 [8, 2048, 16], P(None, ('ctx', 'tp'))
- grad_gate_out: float32 [8, 16, 5632], P(None, None, 'tp')
- grad_up_in: float32 [8, 2048, 16], P(None, ('ctx', 'tp'))
- grad_up_out: float32 [8, 16, 5632], P(None, None, 'tp')
- grad_down_in: float32 [8, 5632, 16], P(None, 'tp')
- grad_down_out: float32 [8, 16, 2048], replicated
The draws below stay inside these ranges and needn't reach their ends.
All inputs are finite; a program needn't handle non-finite values.
Results may differ from the reference program's by a relative error of at most 0.028.
Values may be sent and summed in bfloat16 or wider, within the bound.
A program may use at most 256 MiB of HBM per device.

```python
import jax
import jax.numpy as jnp
from jax import lax

D = 2048
HEADS = 32
KV_HEADS = 4
HEAD_DIM = 64
FF = 5632
RANK = 16
ADAPTERS = 8
SEQS = 4
SEQ_LEN = 2048


def with_ends(array, stream_key, least, largest):
    longest = array.shape.index(max(array.shape))
    spots = []
    for shift in (0, 1):
        where = [jax.random.randint(jax.random.fold_in(stream_key, axis), (), 0, length) for axis, length in enumerate(array.shape)]
        where[longest] = (where[longest] + shift) % array.shape[longest]
        spots.append(tuple(where))
    return array.at[spots[0]].set(least).at[spots[1]].set(largest)


def shard_levels(own_key, extent, cuts, low, high):
    factor_of = 1.0
    for axis_at, blocks in cuts:
        draws = jax.random.uniform(jax.random.fold_in(jax.random.fold_in(own_key, 6), axis_at), (blocks,), jnp.float32, low / len(cuts), high / len(cuts))
        factor_of = factor_of * jnp.repeat(jnp.exp(draws), extent[axis_at] // blocks).reshape((-1,) + (1,) * (len(extent) - 1 - axis_at))
    return factor_of


def gaussian(own_key, shape, deviation, most, split=(), dtype=jnp.bfloat16):
    values = deviation * jax.random.normal(own_key, shape, jnp.float32)
    if split:
        values = values * shard_levels(own_key, shape, split, -0.22, 0.18)
    return jnp.clip(values, -most, most).astype(dtype)


def setup_inputs(seed: int = 0) -> dict:
    arg_keys = jax.random.split(jax.random.key(seed), 27)
    return {
        "tokens_in": gaussian(arg_keys[0], (SEQS, SEQ_LEN, D), 1.0, 6.0, ((1, 8),)),
        "query_weight": gaussian(arg_keys[1], (D, D), D ** -0.5, 0.125, ((0, 8), (1, 4))),
        "key_weight": gaussian(arg_keys[2], (D, KV_HEADS * HEAD_DIM), D ** -0.5, 0.125, ((0, 8), (1, 4))),
        "value_weight": gaussian(arg_keys[3], (D, KV_HEADS * HEAD_DIM), D ** -0.5, 0.125, ((0, 8), (1, 4))),
        "output_projection_matrix": gaussian(arg_keys[4], (D, D), (D // 64) ** -0.5, 1.0, ((0, 4), (1, 8))),
        "gate_weight": gaussian(arg_keys[5], (D, FF), D ** -0.5, 0.125, ((0, 8), (1, 4))),
        "up_weight": gaussian(arg_keys[6], (D, FF), D ** -0.5, 0.125, ((0, 8), (1, 4))),
        "down_projection_matrix": gaussian(arg_keys[7], (FF, D), FF ** -0.5, 0.078125, ((0, 4), (1, 8))),
        "gain_attn": jnp.clip(1.0 + 0.18 * jax.random.normal(arg_keys[8], (D,), jnp.float32), 0.099609375, 1.8984375).astype(jnp.bfloat16),
        "gain_ffn": jnp.clip(1.0 + 0.18 * jax.random.normal(arg_keys[9], (D,), jnp.float32), 0.099609375, 1.8984375).astype(jnp.bfloat16),
        "query_in": gaussian(arg_keys[10], (ADAPTERS, D, RANK), D ** -0.5, 0.125),
        "query_out": gaussian(arg_keys[11], (ADAPTERS, RANK, D), (16 * RANK) ** -0.5, 0.375, ((2, 4),)),
        "key_in": gaussian(arg_keys[12], (ADAPTERS, D, RANK), D ** -0.5, 0.125),
        "key_out": gaussian(arg_keys[13], (ADAPTERS, RANK, KV_HEADS * HEAD_DIM), (16 * RANK) ** -0.5, 0.375, ((2, 4),)),
        "value_in": gaussian(arg_keys[14], (ADAPTERS, D, RANK), D ** -0.5, 0.125),
        "value_out": gaussian(arg_keys[15], (ADAPTERS, RANK, KV_HEADS * HEAD_DIM), (16 * RANK) ** -0.5, 0.375, ((2, 4),)),
        "output_in": gaussian(arg_keys[16], (ADAPTERS, D, RANK), (D // 64) ** -0.5, 1.0, ((1, 4),)),
        "output_adapter_second": gaussian(arg_keys[17], (ADAPTERS, RANK, D), (16 * RANK) ** -0.5, 0.375),
        "gate_in": gaussian(arg_keys[18], (ADAPTERS, D, RANK), D ** -0.5, 0.125),
        "gate_out": gaussian(arg_keys[19], (ADAPTERS, RANK, FF), (16 * RANK) ** -0.5, 0.375, ((2, 4),)),
        "up_in": gaussian(arg_keys[20], (ADAPTERS, D, RANK), D ** -0.5, 0.125),
        "up_out": gaussian(arg_keys[21], (ADAPTERS, RANK, FF), (16 * RANK) ** -0.5, 0.375, ((2, 4),)),
        "down_in": gaussian(arg_keys[22], (ADAPTERS, FF, RANK), FF ** -0.5, 0.078125, ((1, 4),)),
        "down_adapter_second": gaussian(arg_keys[23], (ADAPTERS, RANK, D), (16 * RANK) ** -0.5, 0.375),
        "adapter_index": with_ends(jax.random.randint(arg_keys[24], (SEQS,), 0, ADAPTERS), jax.random.fold_in(arg_keys[24], 1), 0, ADAPTERS - 1).astype(jnp.int32),
        "cotangent": gaussian(arg_keys[25], (SEQS, SEQ_LEN, D), 1.0, 6.0, ((1, 8),)),
    }


@jax.custom_vjp
def low(v):
    return lax.optimization_barrier(v.astype(jnp.bfloat16)).astype(jnp.float32)

@jax.custom_vjp
def low_back(v):
    return v

def low_keep(v):
    return (low(v), None)

def low_pass(kept, grad):
    return (grad,)

def back_keep(v):
    return (v, None)

def back_low(kept, grad):
    return (low(grad),)
low.defvjp(low_keep, low_pass)
low_back.defvjp(back_keep, back_low)
highest_precision = lax.Precision.HIGHEST
eps_norm = 1e-05
theta_base = 10000.0
adapter_scale = 2.0
masked_score = -1e+30

def matrix_product(operand, weight_matrix):
    return jnp.dot(operand, weight_matrix, precision=highest_precision, preferred_element_type=jnp.float32)

def rms_norm(values, gain_vector):
    return values * lax.rsqrt(lax.optimization_barrier(jnp.mean(values * values, axis=-1, keepdims=True)) + eps_norm) * gain_vector

def rotate(values, cosine_part, sine_part):
    half_dim = values.shape[-1] // 2
    first_half = values[..., :half_dim]
    second_half = values[..., half_dim:]
    return jnp.concatenate([first_half * cosine_part - second_half * sine_part, second_half * cosine_part + first_half * sine_part], axis=-1)

def adapted(input_tokens, weight_matrix, squeeze_table, expansion_table):
    reduced_rows = low(matrix_product(input_tokens, squeeze_table))
    return matrix_product(input_tokens, weight_matrix) + adapter_scale * matrix_product(reduced_rows, expansion_table)

def attend(queries, key_rows, value_rows):
    length = queries.shape[0]
    query_block = min(512, length)
    block_count = length // query_block
    group_size = HEADS // KV_HEADS
    score_factor = HEAD_DIM ** (-0.5)
    grouped = queries.reshape(block_count, query_block, KV_HEADS, group_size, HEAD_DIM)
    starts = jnp.arange(block_count).astype(jnp.int32) * query_block
    columns = jnp.arange(length).astype(jnp.int32)

    def one_block(input_tokens):
        block_queries, first_row = input_tokens
        scores = low_back(jnp.einsum('qkgd,pkd->kgqp', block_queries, key_rows, precision=highest_precision) * score_factor)
        positions = first_row + jnp.arange(query_block).astype(jnp.int32)
        allowed = columns[None, :] <= positions[:, None]
        scores = jnp.where(allowed, scores, masked_score)
        probability = jax.nn.softmax(scores, axis=-1)
        return jnp.einsum('kgqp,pkd->qkgd', low(probability), value_rows, precision=highest_precision)
    attention_result = lax.map(jax.checkpoint(one_block), (grouped, starts))
    return attention_result.reshape(length, HEADS * HEAD_DIM)

def layer(tokens, frozen, chosen, cosine_part, sine_part):
    query_weight, key_weight, value_weight, output_projection_matrix, gate_weight, up_weight, down_projection_matrix, gain_attn, gain_ffn = frozen
    query_in, query_out, key_in, key_out, value_in, value_out, output_in, output_adapter_second, gate_in, gate_out, up_in, up_out, down_in, down_adapter_second = chosen
    length = tokens.shape[0]
    normed_one = low(rms_norm(tokens, gain_attn))
    query_pre = low_back(adapted(normed_one, query_weight, query_in, query_out))
    key_pre = low_back(adapted(normed_one, key_weight, key_in, key_out))
    value_pre = low_back(adapted(normed_one, value_weight, value_in, value_out))
    queries = low(rotate(query_pre.reshape(length, HEADS, HEAD_DIM), cosine_part, sine_part))
    key_rows = low(rotate(key_pre.reshape(length, KV_HEADS, HEAD_DIM), cosine_part, sine_part))
    value_rows = low(value_pre.reshape(length, KV_HEADS, HEAD_DIM))
    attention_result = low_back(low(attend(queries, key_rows, value_rows)))
    output_reduction = low_back(low(matrix_product(attention_result, output_in)))
    adapter_branch = low_back(matrix_product(attention_result, output_projection_matrix) + adapter_scale * matrix_product(output_reduction, output_adapter_second))
    residual = tokens + adapter_branch
    normed_two = low(rms_norm(residual, gain_ffn))
    gate_pre = low_back(adapted(normed_two, gate_weight, gate_in, gate_out))
    up_pre = low_back(adapted(normed_two, up_weight, up_in, up_out))
    hidden_state = low(jax.nn.silu(gate_pre) * up_pre)
    down_reduction = low_back(low(matrix_product(hidden_state, down_in)))
    feedforward_branch = low_back(matrix_product(hidden_state, down_projection_matrix) + adapter_scale * matrix_product(down_reduction, down_adapter_second))
    return residual + feedforward_branch

def reference(tokens_in, query_weight, key_weight, value_weight, output_projection_matrix, gate_weight, up_weight, down_projection_matrix, gain_attn, gain_ffn, query_in, query_out, key_in, key_out, value_in, value_out, output_in, output_adapter_second, gate_in, gate_out, up_in, up_out, down_in, down_adapter_second, adapter_index, cotangent):
    frozen = tuple((item.astype(jnp.float32) for item in (query_weight, key_weight, value_weight, output_projection_matrix, gate_weight, up_weight, down_projection_matrix, gain_attn, gain_ffn)))
    adapters = tuple((item.astype(jnp.float32) for item in (query_in, query_out, key_in, key_out, value_in, value_out, output_in, output_adapter_second, gate_in, gate_out, up_in, up_out, down_in, down_adapter_second)))
    length = tokens_in.shape[1]
    positions = jnp.arange(length).astype(jnp.float32)
    frequency = theta_base ** (-(jnp.arange(HEAD_DIM // 2).astype(jnp.float32) * 2.0 / HEAD_DIM))
    angles = positions[:, None] * frequency[None, :]
    cosine_part = jnp.cos(angles)[:, None, :]
    sine_part = jnp.sin(angles)[:, None, :]

    def per_sequence(totals, input_tokens):
        seq_tokens, seq_cotangent, chosen_index = input_tokens

        def forward(tokens, tables):
            chosen = tuple((adapter_table[chosen_index] for adapter_table in tables))
            return layer(tokens, frozen, chosen, cosine_part, sine_part)
        outputs, pullback = jax.vjp(forward, seq_tokens.astype(jnp.float32), adapters)
        grad_seq, grad_tables = pullback(seq_cotangent.astype(jnp.float32))
        totals = tuple((running + increment for running, increment in zip(totals, grad_tables)))
        return (totals, (outputs.astype(jnp.bfloat16), grad_seq.astype(jnp.bfloat16)))
    zero_tables = tuple((jnp.zeros_like(item) for item in adapters))
    adapter_grads, (result_all, grad_all) = lax.scan(per_sequence, zero_tables, (tokens_in, cotangent, adapter_index))
    return (result_all, grad_all, adapter_grads[0], adapter_grads[1], adapter_grads[2], adapter_grads[3], adapter_grads[4], adapter_grads[5], adapter_grads[6], adapter_grads[7], adapter_grads[8], adapter_grads[9], adapter_grads[10], adapter_grads[11], adapter_grads[12], adapter_grads[13])
```

```python
import functools

import jax
import jax.numpy as jnp
from jax import lax
from jax.experimental import pallas as pl
from jax.experimental.pallas import tpu as pltpu
from jax.sharding import PartitionSpec as P

HEAD_DIM = 64
LORA = 128

eps_norm = 1e-05
theta_base = 10000.0
adapter_scale = 2.0
masked_score = -1e30
bf16 = jnp.bfloat16
f32 = jnp.float32
MIB = 1024 * 1024


def nn(a, b):
    return lax.dot_general(a, b, (((1,), (0,)), ((), ())), preferred_element_type=f32)


def nt(a, b):
    return lax.dot_general(a, b, (((1,), (1,)), ((), ())), preferred_element_type=f32)


def turn(a):
    return jnp.transpose(a.astype(f32))


def rms(values):
    return lax.rsqrt(jnp.mean(values * values, axis=-1, keepdims=True) + eps_norm)


def norm_backward(values, gain, inverse, grad):
    weighted = grad * gain
    inner = jnp.mean(weighted * values, axis=-1, keepdims=True)
    return inverse * weighted - values * (inverse * inverse * inverse) * inner


def swap_halves(values):
    width = values.shape[-1]
    lane = lax.broadcasted_iota(jnp.int32, values.shape, 1)
    up = pltpu.roll(values, width - HEAD_DIM // 2, 1)
    down = pltpu.roll(values, HEAD_DIM // 2, 1)
    return jnp.where(lane % HEAD_DIM < HEAD_DIM // 2, up, down)


def params(limit=60, **kw):
    return pltpu.CompilerParams(vmem_limit_bytes=limit * MIB, **kw)


def per_seq(*tail):
    zeros = (0,) * len(tail)
    return pl.BlockSpec((None,) + tail, lambda s, *_: (s,) + zeros)


def whole(*shape):
    zeros = (0,) * len(shape)
    return pl.BlockSpec(shape, lambda s, *_: zeros, pipeline_mode=pl.Buffered(1))


def shaped(shape, dtype):
    return jax.ShapeDtypeStruct(shape, dtype)


def qkv_body(t_ref, g_ref, w_ref, a_ref, b_ref, cos_ref, sin_ref, q_ref, kv_ref, xn_ref, s_ref):
    x = t_ref[...].astype(f32)
    xn = (x * rms(x) * g_ref[...]).astype(bf16)
    xn_ref[...] = xn
    s = nn(xn, a_ref[...]).astype(bf16)
    s_ref[...] = s
    pre = nn(xn, w_ref[...]) + nn(s, b_ref[...])
    rot = (pre * cos_ref[...] + swap_halves(pre) * sin_ref[...]).astype(bf16)
    cut = q_ref.shape[-1]
    q_ref[...] = rot[:, :cut]
    kv_ref[...] = rot[:, cut:]


def split_pairs(kv):
    lane = lax.broadcasted_iota(jnp.int32, kv.shape, 1)
    low = lane < HEAD_DIM
    wide = kv.astype(f32)
    swapped = pltpu.roll(wide, HEAD_DIM, 1)
    zero = jnp.zeros_like(wide)
    keys = (jnp.where(low, wide, zero).astype(bf16), jnp.where(low, zero, swapped).astype(bf16))
    vals = (jnp.where(low, swapped, zero).astype(bf16), jnp.where(low, zero, wide).astype(bf16))
    return keys, vals


def attn_fwd_body(c_ref, q_ref, kv_ref, ob_ref, lse_ref, acc_ref, m_ref, l_ref):
    c = c_ref[0]
    rows = q_ref.shape[0]
    heads = q_ref.shape[1] // HEAD_DIM
    m_ref[...] = jnp.full_like(m_ref, masked_score)
    l_ref[...] = jnp.zeros_like(l_ref)
    acc_ref[...] = jnp.zeros_like(acc_ref)

    def block(j, masked):
        kv = kv_ref[j]
        keys, _ = split_pairs(kv)
        v_t = turn(kv)[HEAD_DIM:].astype(bf16)
        if masked:
            kpos = lax.broadcasted_iota(jnp.int32, (rows, rows), 0)
            qpos = lax.broadcasted_iota(jnp.int32, (rows, rows), 1)
            allowed = kpos <= qpos
        for g in range(heads):
            pair = g // 2
            st = nt(keys[g % 2], q_ref[:, pair * 128 : pair * 128 + 128])
            if masked:
                st = jnp.where(allowed, st, masked_score)
            old = m_ref[g : g + 1, :]
            new = jnp.maximum(old, jnp.max(st, axis=0, keepdims=True))
            p = jnp.exp(st - new)
            fade = jnp.exp(old - new)
            m_ref[g : g + 1, :] = new
            l_ref[g : g + 1, :] = l_ref[g : g + 1, :] * fade + jnp.sum(p, axis=0, keepdims=True)
            acc_ref[g] = acc_ref[g] * fade + nn(v_t, p.astype(bf16))

    def step(j, carry):
        block(j, False)
        return carry

    lax.fori_loop(0, c, step, 0)
    block(c, True)
    total = l_ref[...]
    lse_ref[...] = m_ref[...] + jnp.log(total)
    for pair in range(heads // 2):
        top = acc_ref[2 * pair] / total[2 * pair : 2 * pair + 1, :]
        low = acc_ref[2 * pair + 1] / total[2 * pair + 1 : 2 * pair + 2, :]
        both = jnp.concatenate([top, low], axis=0)
        ob_ref[:, pair * 128 : pair * 128 + 128] = turn(both).astype(bf16)


def attn_bwd_body(
    c_ref, q_ref, kv_ref, do_ref, ob_ref, lse_ref, cos_ref, sin_ref, dq_ref, dkv_ref, dqt_ref, dl_ref
):
    c = c_ref[0]
    rows = q_ref.shape[0]
    heads = q_ref.shape[1] // HEAD_DIM
    dqt_ref[...] = jnp.zeros_like(dqt_ref)
    for pair in range(heads // 2):
        cols = slice(pair * 128, pair * 128 + 128)
        prod = turn(do_ref[:, cols].astype(f32) * ob_ref[:, cols].astype(f32))
        dl_ref[2 * pair : 2 * pair + 1, :] = jnp.sum(prod[:HEAD_DIM], axis=0, keepdims=True)
        dl_ref[2 * pair + 1 : 2 * pair + 2, :] = jnp.sum(prod[HEAD_DIM:], axis=0, keepdims=True)

    def block(j, masked):
        kv = kv_ref[j]
        keys, vals = split_pairs(kv)
        k_t = turn(kv)[:HEAD_DIM].astype(bf16)
        if masked:
            kpos = lax.broadcasted_iota(jnp.int32, (rows, rows), 0)
            qpos = lax.broadcasted_iota(jnp.int32, (rows, rows), 1)
            allowed = kpos <= qpos
        dk = [None, None]
        dv = [None, None]
        for g in range(heads):
            pair = g // 2
            cols = slice(pair * 128, pair * 128 + 128)
            q2 = q_ref[:, cols]
            do2 = do_ref[:, cols]
            st = nt(keys[g % 2], q2)
            p = jnp.exp(st - lse_ref[g : g + 1, :])
            if masked:
                p = jnp.where(allowed, p, 0.0)
            dp = nt(vals[g % 2], do2)
            ds = (p * (dp - dl_ref[g : g + 1, :])).astype(bf16)
            v_part = nn(p.astype(bf16), do2)
            k_part = nn(ds, q2)
            dk[g % 2] = k_part if dk[g % 2] is None else dk[g % 2] + k_part
            dv[g % 2] = v_part if dv[g % 2] is None else dv[g % 2] + v_part
            dqt_ref[g] = dqt_ref[g] + nn(k_t, ds)
        lane = lax.broadcasted_iota(jnp.int32, kv.shape, 1)
        dkeys = dk[0] + pltpu.roll(dk[1], HEAD_DIM, 1)
        dvals = dv[1] + pltpu.roll(dv[0], HEAD_DIM, 1)
        dkv_ref[j] = jnp.where(lane < HEAD_DIM, dkeys, dvals).astype(bf16)

    def step(j, carry):
        block(j, False)
        return carry

    lax.fori_loop(0, c, step, 0)
    block(c, True)

    def clear(j, carry):
        dkv_ref[j] = jnp.zeros(dkv_ref.shape[1:], bf16)
        return carry

    lax.fori_loop(c + 1, dkv_ref.shape[0], clear, 0)
    for pair in range(heads // 2):
        both = jnp.concatenate([dqt_ref[2 * pair], dqt_ref[2 * pair + 1]], axis=0)
        wide = turn(both)
        dq = wide * cos_ref[...] - swap_halves(wide) * sin_ref[...]
        dq_ref[:, pair * 128 : pair * 128 + 128] = dq.astype(bf16)


def mix_body(ob_ref, w_ref, a_ref, out_ref):
    ob = ob_ref[...]
    cut = w_ref.shape[-1]
    out_ref[:, :cut] = nn(ob, w_ref[...]).astype(bf16)
    out_ref[:, cut:] = nn(ob, a_ref[...]).astype(bf16)


def residual_of(t_ref, z_ref, bo_ref):
    width = t_ref.shape[-1]
    so = z_ref[:, width:]
    return t_ref[...].astype(f32) + (z_ref[:, :width].astype(f32) + nn(so, bo_ref[...])), so


def ffn_body(
    t_ref, z_ref, bo_ref, g_ref, agu_ref, wg_ref, wu_ref, bg_ref, bu_ref, wd_ref, ad_ref, bd_ref, dy_ref,
    p2_ref, p3_ref, dbg_ref, dbu_ref, dad_ref,
):
    width = t_ref.shape[-1]
    h, _ = residual_of(t_ref, z_ref, bo_ref)
    xn = (h * rms(h) * g_ref[...]).astype(bf16)
    s = nn(xn, agu_ref[...]).astype(bf16)
    gate = nn(xn, wg_ref[...]) + nn(s, bg_ref[...])
    up = nn(xn, wu_ref[...]) + nn(s, bu_ref[...])
    sig = jax.nn.sigmoid(gate)
    hidden = (gate * sig * up).astype(bf16)
    dy = dy_ref[...]
    dsd = nt(dy, bd_ref[...]).astype(bf16)
    dhid = nt(dy, wd_ref[...]) + nt(dsd, ad_ref[...])
    dgate = (dhid * up * sig * (1.0 + gate * (1.0 - sig))).astype(bf16)
    dup = (dhid * gate * sig).astype(bf16)
    p3_ref[:, :width] = nn(hidden, wd_ref[...]).astype(bf16)
    p3_ref[:, width:] = nn(hidden, ad_ref[...]).astype(bf16)
    p2_ref[:, :width] = (nt(dgate, wg_ref[...]) + nt(dup, wu_ref[...])).astype(bf16)
    p2_ref[:, width:] = (nt(dgate, bg_ref[...]) + nt(dup, bu_ref[...])).astype(bf16)
    s_t = turn(s).astype(bf16)
    rank = dbg_ref.shape[0]
    dbg_ref[...] = (adapter_scale * nn(s_t, dgate)[:rank]).astype(bf16)
    dbu_ref[...] = (adapter_scale * nn(s_t, dup)[rank : 2 * rank]).astype(bf16)
    dad_ref[...] = nn(turn(dsd).astype(bf16), hidden)[:rank].astype(bf16)


def back_body(
    t_ref, z_ref, bo_ref, g_ref, agu_ref, p2_ref, dy_ref, w_ref, ao_ref, ob_ref,
    dh_ref, dob_ref, dbo_ref, dao_ref, dgu_ref,
):
    width = t_ref.shape[-1]
    h, so = residual_of(t_ref, z_ref, bo_ref)
    inverse = rms(h)
    gain = g_ref[...]
    xn = (h * inverse * gain).astype(bf16)
    ds = p2_ref[:, width:]
    dxn = p2_ref[:, :width].astype(f32) + nt(ds, agu_ref[...])
    dh = dy_ref[...].astype(f32) + norm_backward(h, gain, inverse, dxn)
    dz = dh.astype(bf16)
    dh_ref[...] = dz
    dso = nt(dz, bo_ref[...]).astype(bf16)
    dob_ref[...] = (nt(dz, w_ref[...]) + nt(dso, ao_ref[...])).astype(bf16)
    rank = dbo_ref.shape[0]
    dbo_ref[...] = (adapter_scale * nn(turn(so).astype(bf16), dz)[:rank]).astype(bf16)
    dao_ref[...] = nn(turn(dso).astype(bf16), ob_ref[...])[:rank].astype(bf16)
    dgu_ref[...] = nn(turn(ds).astype(bf16), xn)[: 2 * rank].astype(bf16)


def result_body(t_ref, z_ref, bo_ref, p3_ref, bd_ref, dy_ref, out_ref, dbd_ref):
    width = t_ref.shape[-1]
    h, _ = residual_of(t_ref, z_ref, bo_ref)
    sd = p3_ref[:, width:]
    out_ref[...] = (h + (p3_ref[:, :width].astype(f32) + nn(sd, bd_ref[...]))).astype(bf16)
    rank = dbd_ref.shape[0]
    dbd_ref[...] = (adapter_scale * nn(turn(sd).astype(bf16), dy_ref[...])[:rank]).astype(bf16)


def dqkv_body(dq_ref, dkv_ref, cos_ref, sin_ref, w_ref, b_ref, s_ref, p4_ref, db_ref):
    width = w_ref.shape[0]
    dkv = dkv_ref[...]
    back = (dkv * cos_ref[...] - swap_halves(dkv) * sin_ref[...]).astype(bf16)
    both = jnp.concatenate([dq_ref[...], back], axis=1)
    p4_ref[:, :width] = nt(both, w_ref[...]).astype(bf16)
    p4_ref[:, width:] = nt(both, b_ref[...]).astype(bf16)
    db_ref[...] = (adapter_scale * nn(turn(s_ref[...]).astype(bf16), both)[: db_ref.shape[0]]).astype(bf16)


def last_body(t_ref, g_ref, xn_ref, p4_ref, a_ref, dh_ref, out_ref, da_ref):
    width = t_ref.shape[-1]
    x = t_ref[...].astype(f32)
    ds = p4_ref[:, width:]
    dxn = p4_ref[:, :width].astype(f32) + nt(ds, a_ref[...])
    out_ref[...] = (dh_ref[...].astype(f32) + norm_backward(x, g_ref[...], rms(x), dxn)).astype(bf16)
    da_ref[...] = nn(turn(ds).astype(bf16), xn_ref[...])[: da_ref.shape[0]].astype(bf16)


def greet(peers):
    barrier = pltpu.get_barrier_semaphore()
    for peer in peers:
        pl.semaphore_signal(barrier, inc=1, device_id=peer, device_id_type=pl.DeviceIdType.MESH)
    pl.semaphore_wait(barrier, len(peers))


def ring_place(index, n):
    return jnp.where(index % 2 == 0, index // 2, n - 1 - index // 2)


def ring_index(place, n):
    place = lax.rem(place + 2 * n, n)
    return jnp.where(place < n // 2, 2 * place, 2 * (n - 1 - place) + 1)


def remote(src, dst, send, recv, peer):
    return pltpu.make_async_remote_copy(
        src_ref=src, dst_ref=dst, send_sem=send, recv_sem=recv, device_id=peer,
        device_id_type=pl.DeviceIdType.MESH,
    )


def ring_gather_body(n, in_ref, out_ref, send, recv, local):
    me = lax.axis_index("ctx")
    place = ring_place(me, n)
    right = {"ctx": ring_index(place + 1, n)}
    left = {"ctx": ring_index(place - 1, n)}
    greet((left, right))
    mine = pltpu.make_async_copy(in_ref, out_ref.at[me], local)
    mine.start()
    steps = n // 2
    half = in_ref.shape[0] // 2
    for k in range(steps):
        last = k == steps - 1
        copies = []
        for way, peer in ((0, right), (1, left)):
            owner = me if k == 0 else ring_index(place + (k if way else -k), n)
            part = pl.ds(way * half, half) if last else pl.ds(0, 2 * half)
            src = in_ref.at[part] if k == 0 else out_ref.at[owner, part]
            copies.append(
                remote(src, out_ref.at[owner, part], send.at[way, k], recv.at[way, k], peer)
            )
        for copy in copies:
            copy.start()
        for copy in copies:
            copy.wait()
    mine.wait()


def ring_gather(block, n, collective_id):
    return pl.pallas_call(
        functools.partial(ring_gather_body, n),
        out_shape=shaped((n,) + block.shape, block.dtype),
        in_specs=[pl.BlockSpec(memory_space=pltpu.VMEM)],
        out_specs=pl.BlockSpec(memory_space=pltpu.VMEM),
        scratch_shapes=[
            pltpu.SemaphoreType.DMA((2, n // 2)),
            pltpu.SemaphoreType.DMA((2, n // 2)),
            pltpu.SemaphoreType.DMA,
        ],
        compiler_params=params(collective_id=collective_id, has_side_effects=True),
    )(block)


def ring_scatter_body(n, in_ref, out_ref, got, held, send, recv):
    me = lax.axis_index("ctx")
    place = ring_place(me, n)
    right = {"ctx": ring_index(place + 1, n)}
    left = {"ctx": ring_index(place - 1, n)}
    greet((left, right))
    steps = n // 2
    half = in_ref.shape[1] // 2
    for k in range(steps):
        copies = []
        for way, peer in ((0, right), (1, left)):
            ahead = steps - k
            dest = ring_index(place + (-ahead if way else ahead), n)
            mine = pl.ds(way * half, half)
            if k == 0:
                src = in_ref.at[dest, mine]
                dst = got.at[way, 0, mine]
            else:
                if k == 1:
                    rest = pl.ds((1 - way) * half, half)
                    held[way, 1, mine] = (
                        in_ref[dest, mine].astype(f32) + got[way, 0, mine].astype(f32)
                    ).astype(bf16)
                    held[way, 1, rest] = in_ref[dest, rest]
                else:
                    held[way, k] = (
                        in_ref[dest].astype(f32) + got[way, k - 1].astype(f32)
                    ).astype(bf16)
                src = held.at[way, k]
                dst = got.at[way, k]
            copies.append(remote(src, dst, send.at[way, k], recv.at[way, k], peer))
        for copy in copies:
            copy.start()
        for copy in copies:
            copy.wait()
    out_ref[...] = (
        in_ref[me].astype(f32) + got[0, steps - 1].astype(f32) + got[1, steps - 1].astype(f32)
    )


def ring_scatter(blocks, n, collective_id):
    tail = blocks.shape[1:]
    return pl.pallas_call(
        functools.partial(ring_scatter_body, n),
        out_shape=shaped(tail, f32),
        in_specs=[pl.BlockSpec(memory_space=pltpu.VMEM)],
        out_specs=pl.BlockSpec(memory_space=pltpu.VMEM),
        scratch_shapes=[
            pltpu.VMEM((2, n // 2) + tail, blocks.dtype),
            pltpu.VMEM((2, n // 2) + tail, blocks.dtype),
            pltpu.SemaphoreType.DMA((2, n // 2)),
            pltpu.SemaphoreType.DMA((2, n // 2)),
        ],
        compiler_params=params(collective_id=collective_id, has_side_effects=True),
    )(blocks)


def tp_sum_body(chunks, in_ref, out_ref, near, far, mid, send, recv):
    me = lax.axis_index("tp")
    core = lax.rem(me, 2)
    other_core = {"tp": me + 1 - 2 * core}
    other_chip = {"tp": lax.rem(me + 2, 4)}
    greet((other_core, other_chip))
    half = in_ref.shape[0] // chunks // 2

    def rows(i, which):
        return pl.ds(pl.multiple_of((2 * i + which) * half, half), half)

    firsts, seconds, thirds = [], [], []
    for i in range(chunks):
        copy = remote(in_ref.at[rows(i, 1 - core)], near.at[i], send.at[0, i], recv.at[0, i], other_core)
        copy.start()
        firsts.append(copy)
    for i in range(chunks):
        firsts[i].wait_recv()
        mid[i] = (in_ref[rows(i, core), :].astype(f32) + near[i].astype(f32)).astype(bf16)
        copy = remote(mid.at[i], far.at[i], send.at[1, i], recv.at[1, i], other_chip)
        copy.start()
        seconds.append(copy)
    for i in range(chunks):
        seconds[i].wait_recv()
        out_ref[rows(i, core), :] = (mid[i].astype(f32) + far[i].astype(f32)).astype(bf16)
        span = rows(i, core)
        copy = remote(out_ref.at[span], out_ref.at[span], send.at[2, i], recv.at[2, i], other_core)
        copy.start()
        thirds.append(copy)
    for i in range(chunks):
        thirds[i].wait_recv()
        firsts[i].wait_send()
        seconds[i].wait_send()
        thirds[i].wait_send()


def tp_sum(partial, collective_id, chunks=8):
    rows, width = partial.shape
    piece = (chunks, rows // chunks // 2, width)
    return pl.pallas_call(
        functools.partial(tp_sum_body, chunks),
        out_shape=shaped(partial.shape, partial.dtype),
        in_specs=[pl.BlockSpec(memory_space=pltpu.VMEM)],
        out_specs=pl.BlockSpec(memory_space=pltpu.VMEM),
        scratch_shapes=[
            pltpu.VMEM(piece, partial.dtype),
            pltpu.VMEM(piece, partial.dtype),
            pltpu.VMEM(piece, partial.dtype),
            pltpu.SemaphoreType.DMA((3, chunks)),
            pltpu.SemaphoreType.DMA((3, chunks)),
        ],
        compiler_params=params(collective_id=collective_id, has_side_effects=True),
    )(partial)


def per_device(
    tokens_in, query_weight, key_weight, value_weight, output_projection_matrix, gate_weight, up_weight,
    down_projection_matrix, gain_attn, gain_ffn, query_in, query_out, key_in, key_out, value_in, value_out,
    output_in, output_adapter_second, gate_in, gate_out, up_in, up_out, down_in, down_adapter_second,
    adapter_index, cotangent,
):
    seqs, rows, width = tokens_in.shape
    n = lax.axis_size("ctx")
    shards = lax.axis_size("tp")
    me_ctx = lax.axis_index("ctx")
    me_tp = lax.axis_index("tp")
    tables = query_in.shape[0]
    rank = query_in.shape[2]
    q_width = query_weight.shape[1]
    kv_width = key_weight.shape[1]
    heads = q_width // HEAD_DIM
    ff = gate_weight.shape[1]
    all_width = q_width + 2 * kv_width

    w_first = lax.all_gather(
        jnp.concatenate([query_weight, key_weight, value_weight], axis=1), "ctx", axis=0, tiled=True
    )
    w_out = lax.all_gather(output_projection_matrix, "ctx", axis=1, tiled=True)
    w_gate = lax.all_gather(gate_weight, "ctx", axis=0, tiled=True)
    w_up = lax.all_gather(up_weight, "ctx", axis=0, tiled=True)
    w_down = lax.all_gather(down_projection_matrix, "ctx", axis=1, tiled=True)

    def pick(table):
        return jnp.stack([lax.dynamic_index_in_dim(table, adapter_index[s], 0, False) for s in range(seqs)])

    def first(*picked):
        joined = jnp.concatenate([pick(item) for item in picked], axis=2)
        return jnp.pad(joined, ((0, 0), (0, 0), (0, LORA - joined.shape[2])))

    def second(table, at):
        item = pick(table) * jnp.asarray(adapter_scale, bf16)
        return jnp.pad(item, ((0, 0), (at, LORA - at - rank), (0, 0)))

    a_first = first(query_in, key_in, value_in)
    b_first = jnp.concatenate(
        [second(query_out, 0), second(key_out, rank), second(value_out, 2 * rank)], axis=2
    )
    a_gu = first(gate_in, up_in)
    b_gate = second(gate_out, 0)
    b_up = second(up_out, rank)
    a_out = first(output_in)
    b_out = second(output_adapter_second, 0)
    a_down = first(down_in)
    b_down = second(down_adapter_second, 0)
    gain_one = gain_attn.astype(f32)[None, :]
    gain_two = gain_ffn.astype(f32)[None, :]

    lane = jnp.arange(HEAD_DIM)
    frequency = theta_base ** (-((lane % (HEAD_DIM // 2)).astype(f32) * 2.0 / HEAD_DIM))
    position = (me_ctx * rows + jnp.arange(rows, dtype=jnp.int32)).astype(f32)
    angles = position[:, None] * frequency[None, :]
    cosine = jnp.cos(angles)
    sine = jnp.where(lane < HEAD_DIM // 2, -1.0, 1.0)[None, :] * jnp.sin(angles)
    shrink = HEAD_DIM ** (-0.5)
    ones = jnp.ones((rows, kv_width), f32)
    cos_kv = jnp.concatenate([cosine, ones], axis=1)
    sin_kv = jnp.concatenate([sine, jnp.zeros_like(ones)], axis=1)
    cos_q = jnp.tile(cosine * shrink, (1, 2))
    sin_q = jnp.tile(sine * shrink, (1, 2))
    cos_all = jnp.concatenate([jnp.tile(cos_q, (1, heads // 2)), cos_kv], axis=1)
    sin_all = jnp.concatenate([jnp.tile(sin_q, (1, heads // 2)), sin_kv], axis=1)
    place = me_ctx.astype(jnp.int32).reshape(1)

    def call(body, ins, outs, scratch=(), scalars=(), flops=0, limit=60):
        specs = [item[1] for item in ins]
        args = [item[0] for item in ins]
        moved = sum(a.size * a.dtype.itemsize for a in args)
        return pl.pallas_call(
            body,
            out_shape=[shaped(shape, dtype) for shape, dtype, _ in outs],
            grid_spec=pltpu.PrefetchScalarGridSpec(
                num_scalar_prefetch=len(scalars),
                grid=(seqs,),
                in_specs=specs,
                out_specs=[spec for _, _, spec in outs],
                scratch_shapes=list(scratch),
            ),
            cost_estimate=pl.CostEstimate(flops=flops, bytes_accessed=moved, transcendentals=0),
            compiler_params=params(limit, dimension_semantics=("arbitrary",)),
            name=body.__name__,
        )(*scalars, *args)

    row = per_seq(rows, width)
    pay = per_seq(rows, width + LORA)
    total_rows = seqs * rows

    q, kv, xn_one, s_one = call(
        qkv_body,
        [
            (tokens_in, row), (gain_one, whole(1, width)), (w_first, whole(width, all_width)),
            (a_first, per_seq(width, LORA)), (b_first, per_seq(LORA, all_width)),
            (cos_all, whole(rows, all_width)), (sin_all, whole(rows, all_width)),
        ],
        [
            ((seqs, rows, q_width), bf16, per_seq(rows, q_width)),
            ((seqs, rows, 2 * kv_width), bf16, per_seq(rows, 2 * kv_width)),
            ((seqs, rows, width), bf16, row),
            ((seqs, rows, LORA), bf16, per_seq(rows, LORA)),
        ],
        flops=2 * total_rows * width * (all_width + LORA),
    )
    kv_all = ring_gather(kv, n, 1)
    kv_spec = pl.BlockSpec((n, None, rows, 2 * kv_width), lambda s, *_: (0, s, 0, 0))
    stat = per_seq(heads, rows)
    ob, lse = call(
        attn_fwd_body,
        [(q, per_seq(rows, q_width)), (kv_all, kv_spec)],
        [((seqs, rows, q_width), bf16, per_seq(rows, q_width)), ((seqs, heads, rows), f32, stat)],
        scratch=[
            pltpu.VMEM((heads, HEAD_DIM, rows), f32),
            pltpu.VMEM((heads, rows), f32),
            pltpu.VMEM((heads, rows), f32),
        ],
        scalars=(place,),
        flops=4 * total_rows * q_width * rows * n,
    )
    (p1,) = call(
        mix_body,
        [(ob, per_seq(rows, q_width)), (w_out, whole(q_width, width)), (a_out, per_seq(q_width, LORA))],
        [((seqs, rows, width + LORA), bf16, pay)],
        flops=2 * total_rows * q_width * width,
    )
    z = tp_sum(p1.reshape(total_rows, -1), 2).reshape(p1.shape)
    b_out_item = (b_out, per_seq(LORA, width))
    p2, p3, dbg, dbu, dad = call(
        ffn_body,
        [
            (tokens_in, row), (z, pay), b_out_item, (gain_two, whole(1, width)),
            (a_gu, per_seq(width, LORA)), (w_gate, whole(width, ff)), (w_up, whole(width, ff)),
            (b_gate, per_seq(LORA, ff)), (b_up, per_seq(LORA, ff)), (w_down, whole(ff, width)),
            (a_down, per_seq(ff, LORA)), (b_down, per_seq(LORA, width)), (cotangent, row),
        ],
        [
            ((seqs, rows, width + LORA), bf16, pay), ((seqs, rows, width + LORA), bf16, pay),
            ((seqs, rank, ff), bf16, per_seq(rank, ff)), ((seqs, rank, ff), bf16, per_seq(rank, ff)),
            ((seqs, rank, ff), bf16, per_seq(rank, ff)),
        ],
        flops=12 * total_rows * width * ff,
    )
    p2 = tp_sum(p2.reshape(total_rows, -1), 2).reshape(p2.shape)
    dh, dob, dbo, dao, dgu = call(
        back_body,
        [
            (tokens_in, row), (z, pay), b_out_item, (gain_two, whole(1, width)),
            (a_gu, per_seq(width, LORA)), (p2, pay), (cotangent, row), (w_out, whole(q_width, width)),
            (a_out, per_seq(q_width, LORA)), (ob, per_seq(rows, q_width)),
        ],
        [
            ((seqs, rows, width), bf16, row), ((seqs, rows, q_width), bf16, per_seq(rows, q_width)),
            ((seqs, rank, width), bf16, per_seq(rank, width)),
            ((seqs, rank, q_width), bf16, per_seq(rank, q_width)),
            ((seqs, 2 * rank, width), bf16, per_seq(2 * rank, width)),
        ],
        flops=2 * total_rows * q_width * width,
    )
    p3 = lax.psum(p3, "tp")

    def quarter(term):
        cut = term.reshape(seqs, -1, n, shards, width // n // shards)
        cut = lax.dynamic_index_in_dim(cut, me_tp, 3, False)
        return cut.reshape(seqs, -1, rank, width // shards).transpose(0, 2, 1, 3).reshape(seqs, rank, -1)

    early = jnp.concatenate([dbg, dbu, dad, dao, dbo, quarter(dgu)], axis=2)
    early = lax.psum(early, "ctx")

    dq, dkv = call(
        attn_bwd_body,
        [
            (q, per_seq(rows, q_width)), (kv_all, kv_spec), (dob, per_seq(rows, q_width)),
            (ob, per_seq(rows, q_width)), (lse, stat), (cos_q, whole(rows, 128)), (sin_q, whole(rows, 128)),
        ],
        [
            ((seqs, rows, q_width), bf16, per_seq(rows, q_width)),
            ((n, seqs, rows, 2 * kv_width), bf16, kv_spec),
        ],
        scratch=[pltpu.VMEM((heads, HEAD_DIM, rows), f32), pltpu.VMEM((heads, rows), f32)],
        scalars=(place,),
        flops=10 * total_rows * q_width * rows * n,
    )
    dkv = ring_scatter(dkv, n, 3)
    p4, dbf = call(
        dqkv_body,
        [
            (dq, per_seq(rows, q_width)), (dkv, per_seq(rows, 2 * kv_width)),
            (cos_kv, whole(rows, 2 * kv_width)), (sin_kv, whole(rows, 2 * kv_width)),
            (w_first, whole(width, all_width)), (b_first, per_seq(LORA, all_width)),
            (s_one, per_seq(rows, LORA)),
        ],
        [
            ((seqs, rows, width + LORA), bf16, pay),
            ((seqs, 3 * rank, all_width), bf16, per_seq(3 * rank, all_width)),
        ],
        flops=2 * total_rows * width * all_width,
    )
    p4 = tp_sum(p4.reshape(total_rows, -1), 2).reshape(p4.shape)
    result, dbd = call(
        result_body,
        [
            (tokens_in, row), (z, pay), b_out_item, (p3, pay), (b_down, per_seq(LORA, width)),
            (cotangent, row),
        ],
        [((seqs, rows, width), bf16, row), ((seqs, rank, width), bf16, per_seq(rank, width))],
    )
    grad_tokens, dfirst = call(
        last_body,
        [
            (tokens_in, row), (gain_one, whole(1, width)), (xn_one, row), (p4, pay),
            (a_first, per_seq(width, LORA)), (dh, row),
        ],
        [
            ((seqs, rows, width), bf16, row),
            ((seqs, 3 * rank, width), bf16, per_seq(3 * rank, width)),
        ],
    )
    dbq = dbf[:, :rank, :q_width]
    dbk = dbf[:, rank : 2 * rank, q_width : q_width + kv_width]
    dbv = dbf[:, 2 * rank :, q_width + kv_width :]
    late = jnp.concatenate([dbq, dbk, dbv, dbd, quarter(dfirst)], axis=2)
    late = lax.psum(late, "ctx")

    chooser = (
        adapter_index[:, None] == jnp.arange(tables, dtype=jnp.int32)[None, :]
    ).astype(f32)

    def collect(term):
        return jnp.sum(chooser[:, :, None, None] * term.astype(f32)[:, None], axis=0)

    def cuts(packed, sizes):
        out, at = [], 0
        for size in sizes:
            out.append(packed[:, :, at : at + size])
            at += size
        return out

    def own(term):
        part = width // n // shards
        return collect(lax.dynamic_slice_in_dim(term, me_ctx * part, part, 2)).transpose(0, 2, 1)

    quart = width // shards
    e = cuts(early, [ff, ff, ff, q_width, width, quart, quart])
    l = cuts(late, [q_width, kv_width, kv_width, width, quart, quart, quart])
    return (
        result,
        grad_tokens,
        own(l[4]),
        collect(l[0]),
        own(l[5]),
        collect(l[1]),
        own(l[6]),
        collect(l[2]),
        collect(e[3]).transpose(0, 2, 1),
        collect(e[4]),
        own(e[5]),
        collect(e[0]),
        own(e[6]),
        collect(e[1]),
        collect(e[2]).transpose(0, 2, 1),
        collect(l[3]),
    )


def solution(mesh):
    column = P(None, None, "tp")
    split = P(None, ("ctx", "tp"), None)
    return jax.shard_map(
        per_device,
        mesh=mesh,
        in_specs=(
            P(None, "ctx", None), P("ctx", "tp"), P("ctx", "tp"), P("ctx", "tp"), P("tp", "ctx"),
            P("ctx", "tp"), P("ctx", "tp"), P("tp", "ctx"), P(), P(), P(), column, P(), column, P(), column,
            P(None, "tp", None), P(), P(), column, P(), column, P(None, "tp", None), P(), P(),
            P(None, "ctx", None),
        ),
        out_specs=(
            P(None, "ctx", None), P(None, "ctx", None), split, column, split, column, split, column,
            P(None, "tp", None), P(), split, column, split, column, P(None, "tp", None), P(),
        ),
        check_vma=False,
    )
```

```python
import functools

import jax
import jax.numpy as jnp
from jax import lax
from jax.experimental import pallas as pl
from jax.experimental.pallas import tpu as pltpu
from jax.sharding import PartitionSpec as P

HEAD_DIM = 64
LORA = 128

eps_norm = 1e-05
theta_base = 10000.0
adapter_scale = 2.0
masked_score = -1e30
bf16 = jnp.bfloat16
f32 = jnp.float32
MIB = 1024 * 1024


def nn(a, b):
    return lax.dot_general(a, b, (((1,), (0,)), ((), ())), preferred_element_type=f32)


def nt(a, b):
    return lax.dot_general(a, b, (((1,), (1,)), ((), ())), preferred_element_type=f32)


def turn(a):
    return jnp.transpose(a.astype(f32))


def rms(values):
    return lax.rsqrt(jnp.mean(values * values, axis=-1, keepdims=True) + eps_norm)


def norm_backward(values, gain, inverse, grad):
    weighted = grad * gain
    inner = jnp.mean(weighted * values, axis=-1, keepdims=True)
    return inverse * weighted - values * (inverse * inverse * inverse) * inner


def swap_halves(values):
    width = values.shape[-1]
    lane = lax.broadcasted_iota(jnp.int32, values.shape, 1)
    up = pltpu.roll(values, width - HEAD_DIM // 2, 1)
    down = pltpu.roll(values, HEAD_DIM // 2, 1)
    return jnp.where(lane % HEAD_DIM < HEAD_DIM // 2, up, down)


def params(limit=60, **kw):
    return pltpu.CompilerParams(vmem_limit_bytes=limit * MIB, **kw)


def per_seq(*tail):
    zeros = (0,) * len(tail)
    return pl.BlockSpec((None,) + tail, lambda s, *_: (s,) + zeros)


def whole(*shape):
    zeros = (0,) * len(shape)
    return pl.BlockSpec(shape, lambda s, *_: zeros, pipeline_mode=pl.Buffered(1))


def shaped(shape, dtype):
    return jax.ShapeDtypeStruct(shape, dtype)


def ring_place(index, n):
    return jnp.where(index % 2 == 0, index // 2, n - 1 - index // 2)


def ring_index(place, n):
    place = lax.rem(place + 2 * n, n)
    return jnp.where(place < n // 2, 2 * place, 2 * (n - 1 - place) + 1)


def ring_hop(held, n, gate=None):
    order = [2 * p if p < n // 2 else 2 * (n - 1 - p) + 1 for p in range(n)]
    right = [(order[p], order[(p + 1) % n]) for p in range(n)]
    left = [(b, a) for a, b in right]
    pairs = [(chunks[-2], chunks[-1]) if len(chunks) > 1 else (chunks[0],) * 2 for chunks in held]
    if gate is not None:
        pairs, _ = lax.optimization_barrier((pairs, gate))
    for chunks, (ahead, behind) in zip(held, pairs):
        if len(chunks) == n - 1:
            half = ahead.shape[0] // 2
            ahead, behind = ahead[:half], behind[half:]
        chunks.append(lax.ppermute(ahead, "ctx", right))
        chunks.append(lax.ppermute(behind, "ctx", left))


def fill(refs, dst, axis, me, sem, start):
    if len(refs) == 1:
        copy = pltpu.make_async_copy(refs[0], dst, sem.at[0])
        return copy.start() if start else copy.wait()
    n = len(refs) - 1
    place = ring_place(me, n)
    size = dst.shape[axis] // n
    for i, ref in enumerate(refs):
        k = (i + 1) // 2
        way = (i - 1) % 2
        owner = me if k == 0 else ring_index(place + (k if way else -k), n)
        owner = pl.multiple_of(owner * size, size)
        rows = refs[0].shape[0]
        if axis == 0:
            target = dst.at[pl.ds(owner + (way * (rows // 2) if k == n // 2 else 0), ref.shape[0])]
        else:
            top = way * (rows // 2) if k == n // 2 else 0
            target = dst.at[pl.ds(top, ref.shape[0]), pl.ds(owner, size)]
        copy = pltpu.make_async_copy(ref, target, sem.at[i])
        if start:
            copy.start()
        else:
            copy.wait()


def qkv_body(
    c_ref, t_ref, g_ref, w_refs, a_ref, b_ref, cos_ref, sin_ref, q_ref, kv_ref, xn_ref, s_ref, w_ref, sem
):
    @pl.when(pl.program_id(0) == 0)
    def _():
        fill(w_refs, w_ref, 0, c_ref[0], sem, True)
        fill(w_refs, w_ref, 0, c_ref[0], sem, False)

    x = t_ref[...].astype(f32)
    xn = (x * rms(x) * g_ref[...]).astype(bf16)
    xn_ref[...] = xn
    s = nn(xn, a_ref[...]).astype(bf16)
    s_ref[...] = s
    pre = nn(xn, w_ref[...]) + nn(s, b_ref[...])
    rot = (pre * cos_ref[...] + swap_halves(pre) * sin_ref[...]).astype(bf16)
    cut = q_ref.shape[-1]
    q_ref[...] = rot[:, :cut]
    kv_ref[...] = rot[:, cut:]


def split_pairs(kv):
    lane = lax.broadcasted_iota(jnp.int32, kv.shape, 1)
    low = lane < HEAD_DIM
    wide = kv.astype(f32)
    swapped = pltpu.roll(wide, HEAD_DIM, 1)
    zero = jnp.zeros_like(wide)
    keys = (jnp.where(low, wide, zero).astype(bf16), jnp.where(low, zero, swapped).astype(bf16))
    vals = (jnp.where(low, swapped, zero).astype(bf16), jnp.where(low, zero, wide).astype(bf16))
    return keys, vals


def attn_fwd_body(c_ref, q_ref, kv_ref, ob_ref, lse_ref, acc_ref):
    c = c_ref[0]
    rows = q_ref.shape[0]
    heads = q_ref.shape[1] // HEAD_DIM
    acc_ref[...] = jnp.zeros_like(acc_ref)

    def block(j, carry, masked):
        top, total = carry
        kv = kv_ref[j]
        keys, _ = split_pairs(kv)
        v_t = turn(kv)[HEAD_DIM:].astype(bf16)
        if masked:
            kpos = lax.broadcasted_iota(jnp.int32, (rows, rows), 0)
            qpos = lax.broadcasted_iota(jnp.int32, (rows, rows), 1)
            allowed = kpos <= qpos
        scores, tops, sums = [], [], []
        for g in range(heads):
            pair = g // 2
            st = nt(keys[g % 2], q_ref[:, pair * 128 : pair * 128 + 128])
            if masked:
                st = jnp.where(allowed, st, masked_score)
            scores.append(st)
            tops.append(jnp.max(st, axis=0, keepdims=True))
        new = jnp.maximum(top, jnp.concatenate(tops, axis=0))
        fade = jnp.exp(top - new)
        for g in range(heads):
            p = jnp.exp(scores[g] - new[g : g + 1])
            sums.append(jnp.sum(p, axis=0, keepdims=True))
            acc_ref[g] = acc_ref[g] * fade[g : g + 1] + nn(v_t, p.astype(bf16))
        return new, total * fade + jnp.concatenate(sums, axis=0)

    start = (jnp.full((heads, rows), masked_score, f32), jnp.zeros((heads, rows), f32))
    carry = lax.fori_loop(0, c, lambda j, x: block(j, x, False), start)
    top, total = block(c, carry, True)
    lse_ref[...] = top + jnp.log(total)
    for pair in range(heads // 2):
        both = jnp.concatenate(
            [acc_ref[g] / total[g : g + 1] for g in (2 * pair, 2 * pair + 1)], axis=0
        )
        ob_ref[:, pair * 128 : pair * 128 + 128] = turn(both).astype(bf16)


def attn_bwd_body(
    c_ref, q_ref, kv_ref, do_ref, ob_ref, lse_ref, cos_ref, sin_ref, dq_ref, dkv_ref, dqt_ref, dl_ref
):
    c = c_ref[0]
    rows = q_ref.shape[0]
    heads = q_ref.shape[1] // HEAD_DIM
    dqt_ref[...] = jnp.zeros_like(dqt_ref)
    for pair in range(heads // 2):
        cols = slice(pair * 128, pair * 128 + 128)
        prod = turn(do_ref[:, cols].astype(f32) * ob_ref[:, cols].astype(f32))
        dl_ref[2 * pair : 2 * pair + 1, :] = jnp.sum(prod[:HEAD_DIM], axis=0, keepdims=True)
        dl_ref[2 * pair + 1 : 2 * pair + 2, :] = jnp.sum(prod[HEAD_DIM:], axis=0, keepdims=True)

    def block(j, masked):
        kv = kv_ref[j]
        keys, vals = split_pairs(kv)
        k_t = turn(kv)[:HEAD_DIM].astype(bf16)
        if masked:
            kpos = lax.broadcasted_iota(jnp.int32, (rows, rows), 0)
            qpos = lax.broadcasted_iota(jnp.int32, (rows, rows), 1)
            allowed = kpos <= qpos
        dk = [None, None]
        dv = [None, None]
        pieces = []
        for g in range(heads):
            cols = slice(g // 2 * 128, g // 2 * 128 + 128)
            pieces.append((nt(keys[g % 2], q_ref[:, cols]), nt(vals[g % 2], do_ref[:, cols])))
        lows = []
        for g in range(heads):
            st, dp = pieces[g]
            p = jnp.exp(st - lse_ref[g : g + 1, :])
            if masked:
                p = jnp.where(allowed, p, 0.0)
            lows.append((p.astype(bf16), (p * (dp - dl_ref[g : g + 1, :])).astype(bf16)))
        for g in range(heads):
            cols = slice(g // 2 * 128, g // 2 * 128 + 128)
            p, ds = lows[g]
            v_part = nn(p, do_ref[:, cols])
            k_part = nn(ds, q_ref[:, cols])
            dk[g % 2] = k_part if dk[g % 2] is None else dk[g % 2] + k_part
            dv[g % 2] = v_part if dv[g % 2] is None else dv[g % 2] + v_part
            dqt_ref[g] = dqt_ref[g] + nn(k_t, ds)
        lane = lax.broadcasted_iota(jnp.int32, kv.shape, 1)
        dkeys = dk[0] + pltpu.roll(dk[1], HEAD_DIM, 1)
        dvals = dv[1] + pltpu.roll(dv[0], HEAD_DIM, 1)
        dkv_ref[j] = jnp.where(lane < HEAD_DIM, dkeys, dvals).astype(bf16)

    def step(j, carry):
        block(j, False)
        return carry

    lax.fori_loop(0, c, step, 0)
    block(c, True)

    def clear(j, carry):
        dkv_ref[j] = jnp.zeros(dkv_ref.shape[1:], bf16)
        return carry

    lax.fori_loop(c + 1, dkv_ref.shape[0], clear, 0)
    for pair in range(heads // 2):
        both = jnp.concatenate([dqt_ref[2 * pair], dqt_ref[2 * pair + 1]], axis=0)
        wide = turn(both)
        dq = wide * cos_ref[...] - swap_halves(wide) * sin_ref[...]
        dq_ref[:, pair * 128 : pair * 128 + 128] = dq.astype(bf16)


def mix_body(ob_ref, w_ref, a_ref, out_ref):
    ob = ob_ref[...]
    cut = w_ref.shape[-1]
    out_ref[:, :cut] = nn(ob, w_ref[...]).astype(bf16)
    out_ref[:, cut:] = nn(ob, a_ref[...]).astype(bf16)


def own_columns(term, pick_ref, out_ref):
    size = pick_ref.shape[0]
    low = term[: out_ref.shape[1]].astype(bf16)
    for i in range(out_ref.shape[0]):
        out_ref[i] = nn(low[:, i * size : i * size + size], pick_ref[...]).astype(bf16)


def residual_of(t_ref, z_ref, bo_ref):
    width = t_ref.shape[-1]
    z = jnp.where(pl.program_id(0) < pl.num_programs(0) // 2, z_ref[0][...], z_ref[1][...])
    so = z[:, width:]
    return t_ref[...].astype(f32) + (z[:, :width].astype(f32) + nn(so, bo_ref[...])), so


def ffn_body(
    c_ref, t_ref, z_ref, bo_ref, g_ref, agu_ref, wg_refs, wu_refs, bg_ref, bu_ref, wd_refs, ad_ref, bd_ref,
    dy_ref, p2_ref, mine_ref, other_ref, dbg_ref, dbu_ref, dad_ref, wg_ref, wu_ref, wd_ref, p3_ref, sem,
):
    @pl.when(pl.program_id(0) == 0)
    def _():
        for start in (True, False):
            fill(wg_refs, wg_ref, 0, c_ref[0], sem.at[0], start)
            fill(wu_refs, wu_ref, 0, c_ref[0], sem.at[1], start)
            fill(wd_refs, wd_ref, 1, c_ref[0], sem.at[2], start)

    width = t_ref.shape[-1]
    h, _ = residual_of(t_ref, z_ref, bo_ref)
    xn = (h * rms(h) * g_ref[...]).astype(bf16)
    s = nn(xn, agu_ref[...]).astype(bf16)
    gate = nn(xn, wg_ref[...]) + nn(s, bg_ref[...])
    up = nn(xn, wu_ref[...]) + nn(s, bu_ref[...])
    sig = jax.nn.sigmoid(gate)
    hidden = (gate * sig * up).astype(bf16)
    dy = dy_ref[...]
    dsd = nt(dy, bd_ref[...]).astype(bf16)
    dhid = nt(dy, wd_ref[...]) + nt(dsd, ad_ref[...])
    dgate = (dhid * up * sig * (1.0 + gate * (1.0 - sig))).astype(bf16)
    dup = (dhid * gate * sig).astype(bf16)
    p3_ref[:, :width] = nn(hidden, wd_ref[...]).astype(bf16)
    p3_ref[:, width:] = nn(hidden, ad_ref[...]).astype(bf16)
    half = mine_ref.shape[0]
    core = c_ref[1]
    mine_ref[...] = p3_ref[pl.ds(pl.multiple_of(core * half, half), half), :]
    other_ref[...] = p3_ref[pl.ds(pl.multiple_of((1 - core) * half, half), half), :]
    p2_ref[:, :width] = (nt(dgate, wg_ref[...]) + nt(dup, wu_ref[...])).astype(bf16)
    p2_ref[:, width:] = (nt(dgate, bg_ref[...]) + nt(dup, bu_ref[...])).astype(bf16)
    s_t = turn(s).astype(bf16)
    rank = dbg_ref.shape[0]
    dbg_ref[...] = (adapter_scale * nn(s_t, dgate)[:rank]).astype(bf16)
    dbu_ref[...] = (adapter_scale * nn(s_t, dup)[rank : 2 * rank]).astype(bf16)
    dad_ref[...] = nn(turn(dsd).astype(bf16), hidden)[:rank].astype(bf16)


def back_body(
    t_ref, z_ref, bo_ref, g_ref, agu_ref, p2_ref, dy_ref, w_ref, ao_ref, ob_ref, pick_ref,
    dh_ref, dob_ref, dbo_ref, dao_ref, dgu_ref,
):
    width = t_ref.shape[-1]
    h, so = residual_of(t_ref, z_ref, bo_ref)
    inverse = rms(h)
    gain = g_ref[...]
    xn = (h * inverse * gain).astype(bf16)
    ds = p2_ref[:, width:]
    dxn = p2_ref[:, :width].astype(f32) + nt(ds, agu_ref[...])
    dh = dy_ref[...].astype(f32) + norm_backward(h, gain, inverse, dxn)
    dz = dh.astype(bf16)
    dh_ref[...] = dz
    dso = nt(dz, bo_ref[...]).astype(bf16)
    dob_ref[...] = (nt(dz, w_ref[...]) + nt(dso, ao_ref[...])).astype(bf16)
    rank = dbo_ref.shape[0]
    dbo_ref[...] = (adapter_scale * nn(turn(so).astype(bf16), dz)[:rank]).astype(bf16)
    dao_ref[...] = nn(turn(dso).astype(bf16), ob_ref[...])[:rank].astype(bf16)
    own_columns(nn(turn(ds).astype(bf16), xn), pick_ref, dgu_ref)


def result_body(c_ref, t_ref, z_ref, bo_ref, near_ref, far_ref, bd_ref, dy_ref, out_ref, dbd_ref, p3_ref):
    half = near_ref.shape[0]
    core = c_ref[1]
    p3_ref[pl.ds(pl.multiple_of(core * half, half), half), :] = near_ref[...]
    p3_ref[pl.ds(pl.multiple_of((1 - core) * half, half), half), :] = far_ref[...]
    width = t_ref.shape[-1]
    h, _ = residual_of(t_ref, z_ref, bo_ref)
    sd = p3_ref[:, width:]
    out_ref[...] = (h + (p3_ref[:, :width].astype(f32) + nn(sd, bd_ref[...]))).astype(bf16)
    rank = dbd_ref.shape[0]
    dbd_ref[...] = (adapter_scale * nn(turn(sd).astype(bf16), dy_ref[...])[:rank]).astype(bf16)


def dqkv_body(c_ref, dq_ref, dkv_ref, cos_ref, sin_ref, w_refs, b_ref, s_ref, p4_ref, db_ref, w_ref, sem):
    @pl.when(pl.program_id(0) == 0)
    def _():
        fill(w_refs, w_ref, 0, c_ref[0], sem, True)
        fill(w_refs, w_ref, 0, c_ref[0], sem, False)

    width = w_ref.shape[0]
    dkv = dkv_ref[...]
    back = (dkv * cos_ref[...] - swap_halves(dkv) * sin_ref[...]).astype(bf16)
    both = jnp.concatenate([dq_ref[...], back], axis=1)
    p4_ref[:, :width] = nt(both, w_ref[...]).astype(bf16)
    p4_ref[:, width:] = nt(both, b_ref[...]).astype(bf16)
    db_ref[...] = (adapter_scale * nn(turn(s_ref[...]).astype(bf16), both)[: db_ref.shape[0]]).astype(bf16)


def last_body(t_ref, g_ref, xn_ref, p4_ref, a_ref, dh_ref, pick_ref, out_ref, da_ref):
    width = t_ref.shape[-1]
    x = t_ref[...].astype(f32)
    ds = p4_ref[:, width:]
    dxn = p4_ref[:, :width].astype(f32) + nt(ds, a_ref[...])
    out_ref[...] = (dh_ref[...].astype(f32) + norm_backward(x, g_ref[...], rms(x), dxn)).astype(bf16)
    own_columns(nn(turn(ds).astype(bf16), xn_ref[...]), pick_ref, da_ref)


def greet(peers):
    barrier = pltpu.get_barrier_semaphore()
    for peer in peers:
        pl.semaphore_signal(barrier, inc=1, device_id=peer, device_id_type=pl.DeviceIdType.MESH)
    pl.semaphore_wait(barrier, len(peers))


def remote(src, dst, send, recv, peer):
    return pltpu.make_async_remote_copy(
        src_ref=src, dst_ref=dst, send_sem=send, recv_sem=recv, device_id=peer,
        device_id_type=pl.DeviceIdType.MESH,
    )


def ring_gather_body(n, in_ref, out_ref, send, recv, local):
    me = lax.axis_index("ctx")
    place = ring_place(me, n)
    right = {"ctx": ring_index(place + 1, n)}
    left = {"ctx": ring_index(place - 1, n)}
    greet((left, right))
    mine = pltpu.make_async_copy(in_ref, out_ref.at[me], local)
    mine.start()
    steps = n // 2
    half = in_ref.shape[0] // 2
    for k in range(steps):
        last = k == steps - 1
        copies = []
        for way, peer in ((0, right), (1, left)):
            owner = me if k == 0 else ring_index(place + (k if way else -k), n)
            part = pl.ds(way * half, half) if last else pl.ds(0, 2 * half)
            src = in_ref.at[part] if k == 0 else out_ref.at[owner, part]
            copies.append(
                remote(src, out_ref.at[owner, part], send.at[way, k], recv.at[way, k], peer)
            )
        for copy in copies:
            copy.start()
        for copy in copies:
            copy.wait()
    mine.wait()


def ring_gather(block, n, collective_id):
    return pl.pallas_call(
        functools.partial(ring_gather_body, n),
        out_shape=shaped((n,) + block.shape, block.dtype),
        in_specs=[pl.BlockSpec(memory_space=pltpu.VMEM)],
        out_specs=pl.BlockSpec(memory_space=pltpu.VMEM),
        scratch_shapes=[
            pltpu.SemaphoreType.DMA((2, n // 2)),
            pltpu.SemaphoreType.DMA((2, n // 2)),
            pltpu.SemaphoreType.DMA,
        ],
        compiler_params=params(collective_id=collective_id, has_side_effects=True),
    )(block)


def ring_scatter_body(n, in_ref, out_ref, got, held, send, recv):
    me = lax.axis_index("ctx")
    place = ring_place(me, n)
    right = {"ctx": ring_index(place + 1, n)}
    left = {"ctx": ring_index(place - 1, n)}
    greet((left, right))
    steps = n // 2
    half = in_ref.shape[1] // 2
    for k in range(steps):
        copies = []
        for way, peer in ((0, right), (1, left)):
            ahead = steps - k
            dest = ring_index(place + (-ahead if way else ahead), n)
            mine = pl.ds(way * half, half)
            if k == 0:
                src = in_ref.at[dest, mine]
                dst = got.at[way, 0, mine]
            else:
                if k == 1:
                    rest = pl.ds((1 - way) * half, half)
                    held[way, 1, mine] = (
                        in_ref[dest, mine].astype(f32) + got[way, 0, mine].astype(f32)
                    ).astype(bf16)
                    held[way, 1, rest] = in_ref[dest, rest]
                else:
                    held[way, k] = (
                        in_ref[dest].astype(f32) + got[way, k - 1].astype(f32)
                    ).astype(bf16)
                src = held.at[way, k]
                dst = got.at[way, k]
            copies.append(remote(src, dst, send.at[way, k], recv.at[way, k], peer))
        for copy in copies:
            copy.start()
        for copy in copies:
            copy.wait()
    out_ref[...] = (
        in_ref[me].astype(f32) + got[0, steps - 1].astype(f32) + got[1, steps - 1].astype(f32)
    )


def ring_scatter(blocks, n, collective_id):
    tail = blocks.shape[1:]
    return pl.pallas_call(
        functools.partial(ring_scatter_body, n),
        out_shape=shaped(tail, f32),
        in_specs=[pl.BlockSpec(memory_space=pltpu.VMEM)],
        out_specs=pl.BlockSpec(memory_space=pltpu.VMEM),
        scratch_shapes=[
            pltpu.VMEM((2, n // 2) + tail, blocks.dtype),
            pltpu.VMEM((2, n // 2) + tail, blocks.dtype),
            pltpu.SemaphoreType.DMA((2, n // 2)),
            pltpu.SemaphoreType.DMA((2, n // 2)),
        ],
        compiler_params=params(collective_id=collective_id, has_side_effects=True),
    )(blocks)


def tp_sum_body(chunks, in_ref, out_ref, near, far, mid, send, recv):
    me = lax.axis_index("tp")
    core = lax.rem(me, 2)
    other_core = {"tp": me + 1 - 2 * core}
    other_chip = {"tp": lax.rem(me + 2, 4)}
    greet((other_core, other_chip))
    half = in_ref.shape[0] // chunks // 2

    def rows(i, which):
        return pl.ds(pl.multiple_of((2 * i + which) * half, half), half)

    firsts, seconds, thirds = [], [], []
    for i in range(chunks):
        copy = remote(in_ref.at[rows(i, 1 - core)], near.at[i], send.at[0, i], recv.at[0, i], other_core)
        copy.start()
        firsts.append(copy)
    for i in range(chunks):
        firsts[i].wait_recv()
        mid[i] = (in_ref[rows(i, core), :].astype(f32) + near[i].astype(f32)).astype(bf16)
        copy = remote(mid.at[i], far.at[i], send.at[1, i], recv.at[1, i], other_chip)
        copy.start()
        seconds.append(copy)
    for i in range(chunks):
        seconds[i].wait_recv()
        out_ref[rows(i, core), :] = (mid[i].astype(f32) + far[i].astype(f32)).astype(bf16)
        span = rows(i, core)
        copy = remote(out_ref.at[span], out_ref.at[span], send.at[2, i], recv.at[2, i], other_core)
        copy.start()
        thirds.append(copy)
    for i in range(chunks):
        thirds[i].wait_recv()
        firsts[i].wait_send()
        seconds[i].wait_send()
        thirds[i].wait_send()


def tp_sum(partial, collective_id, chunks=8):
    rows, width = partial.shape
    piece = (chunks, rows // chunks // 2, width)
    return pl.pallas_call(
        functools.partial(tp_sum_body, chunks),
        out_shape=shaped(partial.shape, partial.dtype),
        in_specs=[pl.BlockSpec(memory_space=pltpu.VMEM)],
        out_specs=pl.BlockSpec(memory_space=pltpu.VMEM),
        scratch_shapes=[
            pltpu.VMEM(piece, partial.dtype),
            pltpu.VMEM(piece, partial.dtype),
            pltpu.VMEM(piece, partial.dtype),
            pltpu.SemaphoreType.DMA((3, chunks)),
            pltpu.SemaphoreType.DMA((3, chunks)),
        ],
        compiler_params=params(collective_id=collective_id, has_side_effects=True),
    )(partial)


def per_device(
    tokens_in, query_weight, key_weight, value_weight, output_projection_matrix, gate_weight, up_weight,
    down_projection_matrix, gain_attn, gain_ffn, query_in, query_out, key_in, key_out, value_in, value_out,
    output_in, output_adapter_second, gate_in, gate_out, up_in, up_out, down_in, down_adapter_second,
    adapter_index, cotangent,
):
    seqs, rows, width = tokens_in.shape
    n = lax.axis_size("ctx")
    shards = lax.axis_size("tp")
    me_ctx = lax.axis_index("ctx")
    me_tp = lax.axis_index("tp")
    tables = query_in.shape[0]
    rank = query_in.shape[2]
    q_width = query_weight.shape[1]
    kv_width = key_weight.shape[1]
    heads = q_width // HEAD_DIM
    ff = gate_weight.shape[1]
    all_width = q_width + 2 * kv_width

    def pick(table):
        return jnp.stack([lax.dynamic_index_in_dim(table, adapter_index[s], 0, False) for s in range(seqs)])

    def first(*picked):
        joined = jnp.concatenate([pick(item) for item in picked], axis=2)
        return jnp.pad(joined, ((0, 0), (0, 0), (0, LORA - joined.shape[2])))

    def second(table, at):
        item = pick(table) * jnp.asarray(adapter_scale, bf16)
        return jnp.pad(item, ((0, 0), (at, LORA - at - rank), (0, 0)))

    a_first = first(query_in, key_in, value_in)
    b_first = jnp.concatenate(
        [second(query_out, 0), second(key_out, rank), second(value_out, 2 * rank)], axis=2
    )
    a_gu = first(gate_in, up_in)
    b_gate = second(gate_out, 0)
    b_up = second(up_out, rank)
    a_out = first(output_in)
    b_out = second(output_adapter_second, 0)
    a_down = first(down_in)
    b_down = second(down_adapter_second, 0)
    gain_one = gain_attn.astype(f32)[None, :]
    gain_two = gain_ffn.astype(f32)[None, :]

    lane = jnp.arange(HEAD_DIM)
    frequency = theta_base ** (-((lane % (HEAD_DIM // 2)).astype(f32) * 2.0 / HEAD_DIM))
    position = (me_ctx * rows + jnp.arange(rows, dtype=jnp.int32)).astype(f32)
    angles = position[:, None] * frequency[None, :]
    cosine = jnp.cos(angles)
    sine = jnp.where(lane < HEAD_DIM // 2, -1.0, 1.0)[None, :] * jnp.sin(angles)
    shrink = HEAD_DIM ** (-0.5)
    ones = jnp.ones((rows, kv_width), f32)
    cos_kv = jnp.concatenate([cosine, ones], axis=1)
    sin_kv = jnp.concatenate([sine, jnp.zeros_like(ones)], axis=1)
    cos_q = jnp.tile(cosine * shrink, (1, 2))
    sin_q = jnp.tile(sine * shrink, (1, 2))
    cos_all = jnp.concatenate([jnp.tile(cos_q, (1, heads // 2)), cos_kv], axis=1)
    sin_all = jnp.concatenate([jnp.tile(sin_q, (1, heads // 2)), sin_kv], axis=1)
    place = jnp.stack([me_ctx.astype(jnp.int32), lax.rem(me_tp, 2).astype(jnp.int32)])
    part = width // n
    pick_own = (
        jnp.arange(part)[:, None] == me_tp * (part // shards) + jnp.arange(part // shards)[None, :]
    ).astype(bf16)
    pick_item = (pick_own, whole(part, part // shards))
    ring_sem = pltpu.SemaphoreType.DMA((n + 1,))

    hops = n // 2
    w_first = [jnp.concatenate([query_weight, key_weight, value_weight], axis=1)]
    made = [
        (a_gu, b_gate, b_up, pick_own), (a_down, b_down, a_out, b_out, a_first),
        (b_first, cos_all, sin_all, cos_kv, sin_kv, cos_q, sin_q, gain_one, gain_two),
    ]
    for k in range(hops):
        ring_hop([w_first], n, made[k - 1] if 0 < k <= len(made) else None)
    w_gate, w_up, w_down = [gate_weight], [up_weight], [down_projection_matrix]
    travel = [w_up, w_down, w_gate]
    if part % 128:
        travel = [w_up, w_gate]
        w_down = [lax.all_gather(down_projection_matrix, "ctx", axis=1, tiled=True)]
    ring_hop([w_gate], n, tuple(w_first))

    def spread(chunks):
        return (tuple(chunks), tuple(pl.BlockSpec(memory_space=pl.ANY) for _ in chunks))

    def blocks_of(count):
        return pl.BlockSpec((n, None, count, part // shards), lambda s, *_: (0, s, 0, 0))

    def call(body, ins, outs, scratch=(), scalars=(), flops=0, limit=60, steps=seqs):
        specs = [item[1] for item in ins]
        args = [item[0] for item in ins]
        moved = sum(a.size * a.dtype.itemsize for a in jax.tree.leaves(args))
        return pl.pallas_call(
            body,
            out_shape=[shaped(shape, dtype) for shape, dtype, _ in outs],
            grid_spec=pltpu.PrefetchScalarGridSpec(
                num_scalar_prefetch=len(scalars),
                grid=(steps,),
                in_specs=specs,
                out_specs=[spec for _, _, spec in outs],
                scratch_shapes=list(scratch),
            ),
            cost_estimate=pl.CostEstimate(flops=flops, bytes_accessed=moved, transcendentals=0),
            compiler_params=params(limit, dimension_semantics=("arbitrary",)),
            name=body.__name__,
        )(*scalars, *args)

    row = per_seq(rows, width)
    pay = per_seq(rows, width + LORA)
    total_rows = seqs * rows

    q, kv, xn_one, s_one = call(
        qkv_body,
        [
            (tokens_in, row), (gain_one, whole(1, width)), spread(w_first),
            (a_first, per_seq(width, LORA)), (b_first, per_seq(LORA, all_width)),
            (cos_all, whole(rows, all_width)), (sin_all, whole(rows, all_width)),
        ],
        [
            ((seqs, rows, q_width), bf16, per_seq(rows, q_width)),
            ((seqs, rows, 2 * kv_width), bf16, per_seq(rows, 2 * kv_width)),
            ((seqs, rows, width), bf16, row),
            ((seqs, rows, LORA), bf16, per_seq(rows, LORA)),
        ],
        scratch=[pltpu.VMEM((width, all_width), bf16), ring_sem],
        scalars=(place,),
        flops=2 * total_rows * width * (all_width + LORA),
    )
    kv, _ = lax.optimization_barrier((kv, tuple(w_gate)))
    kv_all = ring_gather(kv, n, 1)
    ring_hop(travel, n, kv_all)
    gated, _ = lax.optimization_barrier((output_projection_matrix, kv_all))
    w_out = lax.all_gather(gated, "ctx", axis=1, tiled=True)
    kv_spec = pl.BlockSpec((n, None, rows, 2 * kv_width), lambda s, *_: (0, s, 0, 0))
    stat = per_seq(heads, rows)
    mixes, obs, lses = [], [], []
    for at in range(seqs):
        one = pl.BlockSpec((None, rows, q_width), lambda s, *_, at=at: (at, 0, 0))
        pair = pl.BlockSpec((n, None, rows, 2 * kv_width), lambda s, *_, at=at: (0, at, 0, 0))
        ob, lse = call(
            attn_fwd_body,
            [(q, one), (kv_all, pair)],
            [((1, rows, q_width), bf16, per_seq(rows, q_width)), ((1, heads, rows), f32, stat)],
            scratch=[pltpu.VMEM((heads, HEAD_DIM, rows), f32)],
            scalars=(place,),
            flops=4 * rows * q_width * rows * n,
            steps=1,
        )
        obs.append(ob)
        lses.append(lse)
    ring_hop(travel, n, tuple(obs))
    ob = jnp.concatenate(obs)
    lse = jnp.concatenate(lses)
    part_seqs = seqs // 2
    zs = []
    for at in (0, part_seqs):
        piece = pl.BlockSpec((None, rows, q_width), lambda s, *_, at=at: (s + at, 0, 0))
        factor = pl.BlockSpec((None, q_width, LORA), lambda s, *_, at=at: (s + at, 0, 0))
        (p1,) = call(
            mix_body,
            [(ob, piece), (w_out, whole(q_width, width)), (a_out, factor)],
            [((part_seqs, rows, width + LORA), bf16, pay)],
            flops=rows * part_seqs * 2 * q_width * width,
            steps=part_seqs,
        )
        if zs:
            p1, _ = lax.optimization_barrier((p1, zs[0]))
        zs.append(tp_sum(p1.reshape(part_seqs * rows, -1), 5, 4).reshape(p1.shape))
        if at == 0:
            ring_hop(travel, n, zs[0])
    while len(w_up) < n + 1:
        ring_hop([item for item in travel if len(item) < n + 1], n, zs[1])
    low_half = pl.BlockSpec(
        (None, rows, width + LORA), lambda s, *_: (jnp.minimum(s, part_seqs - 1), 0, 0)
    )
    high_half = pl.BlockSpec(
        (None, rows, width + LORA), lambda s, *_: (jnp.maximum(s - part_seqs, 0), 0, 0)
    )
    z_item = (tuple(zs), (low_half, high_half))
    b_out_item = (b_out, per_seq(LORA, width))
    half_pay = per_seq(rows // 2, width + LORA)
    p2, p3_mine, p3_other, dbg, dbu, dad = call(
        ffn_body,
        [
            (tokens_in, row), z_item, b_out_item, (gain_two, whole(1, width)),
            (a_gu, per_seq(width, LORA)), spread(w_gate), spread(w_up),
            (b_gate, per_seq(LORA, ff)), (b_up, per_seq(LORA, ff)), spread(w_down),
            (a_down, per_seq(ff, LORA)), (b_down, per_seq(LORA, width)), (cotangent, row),
        ],
        [
            ((seqs, rows, width + LORA), bf16, pay), ((seqs, rows // 2, width + LORA), bf16, half_pay),
            ((seqs, rows // 2, width + LORA), bf16, half_pay),
            ((seqs, rank, ff), bf16, per_seq(rank, ff)), ((seqs, rank, ff), bf16, per_seq(rank, ff)),
            ((seqs, rank, ff), bf16, per_seq(rank, ff)),
        ],
        scratch=[
            pltpu.VMEM((width, ff), bf16), pltpu.VMEM((width, ff), bf16), pltpu.VMEM((ff, width), bf16),
            pltpu.VMEM((rows, width + LORA), bf16), pltpu.SemaphoreType.DMA((3, n + 1)),
        ],
        scalars=(place,),
        flops=12 * total_rows * width * ff,
    )
    p2 = tp_sum(p2.reshape(total_rows, -1), 2).reshape(p2.shape)
    dh, dob, dbo, dao, dgu = call(
        back_body,
        [
            (tokens_in, row), z_item, b_out_item, (gain_two, whole(1, width)),
            (a_gu, per_seq(width, LORA)), (p2, pay), (cotangent, row), (w_out, whole(q_width, width)),
            (a_out, per_seq(q_width, LORA)), (ob, per_seq(rows, q_width)), pick_item,
        ],
        [
            ((seqs, rows, width), bf16, row), ((seqs, rows, q_width), bf16, per_seq(rows, q_width)),
            ((seqs, rank, width), bf16, per_seq(rank, width)),
            ((seqs, rank, q_width), bf16, per_seq(rank, q_width)),
            ((n, seqs, 2 * rank, part // shards), bf16, blocks_of(2 * rank)),
        ],
        flops=2 * total_rows * q_width * width,
    )
    swap_core = [(t, t + 1 - 2 * (t % 2)) for t in range(shards)]
    swap_chip = [(t, (t + 2) % shards) for t in range(shards)]

    def add(a, b):
        return (a.astype(f32) + b.astype(f32)).astype(bf16)

    p3_near, p3_mine, _ = lax.optimization_barrier(
        (lax.ppermute(p3_other, "tp", swap_core), p3_mine, p2)
    )
    p3_half = add(p3_mine, p3_near)
    p3_far = lax.ppermute(p3_half, "tp", swap_chip)

    early = lax.psum(jnp.concatenate([dbg, dbu, dad, dao, dbo], axis=2), "ctx")

    dq, dkv = call(
        attn_bwd_body,
        [
            (q, per_seq(rows, q_width)), (kv_all, kv_spec), (dob, per_seq(rows, q_width)),
            (ob, per_seq(rows, q_width)), (lse, stat), (cos_q, whole(rows, 128)), (sin_q, whole(rows, 128)),
        ],
        [
            ((seqs, rows, q_width), bf16, per_seq(rows, q_width)),
            ((n, seqs, rows, 2 * kv_width), bf16, kv_spec),
        ],
        scratch=[pltpu.VMEM((heads, HEAD_DIM, rows), f32), pltpu.VMEM((heads, rows), f32)],
        scalars=(place,),
        flops=10 * total_rows * q_width * rows * n,
    )
    p3_far, p3_half, _ = lax.optimization_barrier((p3_far, p3_half, dq))
    p3_half = add(p3_half, p3_far)
    p3_back = lax.ppermute(p3_half, "tp", swap_core)
    dkv = ring_scatter(dkv, n, 3)
    p4, dbf = call(
        dqkv_body,
        [
            (dq, per_seq(rows, q_width)), (dkv, per_seq(rows, 2 * kv_width)),
            (cos_kv, whole(rows, 2 * kv_width)), (sin_kv, whole(rows, 2 * kv_width)),
            spread(w_first), (b_first, per_seq(LORA, all_width)),
            (s_one, per_seq(rows, LORA)),
        ],
        [
            ((seqs, rows, width + LORA), bf16, pay),
            ((seqs, 3 * rank, all_width), bf16, per_seq(3 * rank, all_width)),
        ],
        scratch=[pltpu.VMEM((width, all_width), bf16), ring_sem],
        scalars=(place,),
        flops=2 * total_rows * width * all_width,
    )
    result, dbd = call(
        result_body,
        [
            (tokens_in, row), z_item, b_out_item, (p3_half, half_pay), (p3_back, half_pay),
            (b_down, per_seq(LORA, width)), (cotangent, row),
        ],
        [((seqs, rows, width), bf16, row), ((seqs, rank, width), bf16, per_seq(rank, width))],
        scratch=[pltpu.VMEM((rows, width + LORA), bf16)],
        scalars=(place,),
    )
    dbq = dbf[:, :rank, :q_width]
    dbk = dbf[:, rank : 2 * rank, q_width : q_width + kv_width]
    dbv = dbf[:, 2 * rank :, q_width + kv_width :]
    late, early = lax.optimization_barrier((jnp.concatenate([dbq, dbk, dbv, dbd], axis=2), early))
    late = lax.psum(late, "ctx")
    p4, _ = lax.optimization_barrier((p4, dbd))
    p4 = tp_sum(p4.reshape(total_rows, -1), 2).reshape(p4.shape)
    grad_tokens, dfirst = call(
        last_body,
        [
            (tokens_in, row), (gain_one, whole(1, width)), (xn_one, row), (p4, pay),
            (a_first, per_seq(width, LORA)), (dh, row), pick_item,
        ],
        [
            ((seqs, rows, width), bf16, row),
            ((n, seqs, 3 * rank, part // shards), bf16, blocks_of(3 * rank)),
        ],
    )
    firsts = jnp.concatenate([dfirst, dgu], axis=2)
    firsts = ring_scatter(firsts.reshape(n, -1, part // shards), n, 4).reshape(seqs, -1, part // shards)

    chooser = (
        adapter_index[:, None] == jnp.arange(tables, dtype=jnp.int32)[None, :]
    ).astype(f32)

    def collect(term):
        return jnp.sum(chooser[:, :, None, None] * term.astype(f32)[:, None], axis=0)

    def cuts(packed, sizes):
        out, at = [], 0
        for size in sizes:
            out.append(packed[:, :, at : at + size])
            at += size
        return out

    def own(at):
        return collect(firsts[:, at * rank : (at + 1) * rank]).transpose(0, 2, 1)

    e = cuts(early, [ff, ff, ff, q_width, width])
    l = cuts(late, [q_width, kv_width, kv_width, width])
    return (
        result,
        grad_tokens,
        own(0),
        collect(l[0]),
        own(1),
        collect(l[1]),
        own(2),
        collect(l[2]),
        collect(e[3]).transpose(0, 2, 1),
        collect(e[4]),
        own(3),
        collect(e[0]),
        own(4),
        collect(e[1]),
        collect(e[2]).transpose(0, 2, 1),
        collect(l[3]),
    )


def solution(mesh):
    column = P(None, None, "tp")
    split = P(None, ("ctx", "tp"), None)
    return jax.shard_map(
        per_device,
        mesh=mesh,
        in_specs=(
            P(None, "ctx", None), P("ctx", "tp"), P("ctx", "tp"), P("ctx", "tp"), P("tp", "ctx"),
            P("ctx", "tp"), P("ctx", "tp"), P("tp", "ctx"), P(), P(), P(), column, P(), column, P(), column,
            P(None, "tp", None), P(), P(), column, P(), column, P(None, "tp", None), P(), P(),
            P(None, "ctx", None),
        ),
        out_specs=(
            P(None, "ctx", None), P(None, "ctx", None), split, column, split, column, split, column,
            P(None, "tp", None), P(), split, column, split, column, P(None, "tp", None), P(),
        ),
        check_vma=False,
    )
```
